32 devices in a mesh: row: 4 (over x, core), col: 8 (over z, y).
Axes of the slice: x: 2, y: 2, z: 4, core: 2. Of those that a mesh axis runs over, the one named last changes fastest.
Arguments:
- ancestor_order: int32 [2, 48], replicated, may hold values from 0 to 47, each once within a row
- factor_rows: bfloat16 [2, 24576, 512], P(None, ('row', 'col')), may hold values from -0.0390625 to 0.0390625
- factor_inverse: bfloat16 [2, 512, 512], replicated
- ancestor_inverse: bfloat16 [24576, 24576], P('col', 'row'), may hold values from -6 to 6
- diagonal_inverse: float32 [2, 512, 512], P(None, None, 'row'), may hold values from -6 to 6
Outputs:
- offdiag_inverse: bfloat16 [2, 24576, 512], P(None, 'col', 'row')
- diag_updated: float32 [2, 512, 512], P(None, None, 'row')
The draws below stay inside these ranges and needn't reach their ends.
Inputs may be any that keep to these rules, and one draw needn't show every extreme that they name: `ancestor_order`: each row lists every ancestor block once; its first 40 entries are the blocks coupled to that supernode.
All inputs are finite; a program needn't handle non-finite values.
Results may differ from the reference program's by a relative error of at most 0.011.
Values may be sent and summed in bfloat16 or wider, within the bound.
A program may use at most 128 MiB of HBM per device.

```python
import math
import jax
import jax.numpy as jnp
from jax import lax

B = 512
NA = 48
NSEL = 40
NSUP = 2


def draw_factor_inverse(key, part):
    noise = jax.random.normal(key, (NSUP, B, B), jnp.float32) * (0.6 / math.sqrt(B))
    lower = jnp.tril(noise, -1) + jnp.eye(B, dtype=jnp.float32)[None, :, :]
    return lower.astype(jnp.bfloat16)


def steps_of(key, dims, cuts, low, high):
    loudness = 1.0
    for position, blocks in cuts:
        heights = jax.random.uniform(jax.random.fold_in(jax.random.fold_in(key, 6), position), (blocks,), jnp.float32, low / len(cuts), high / len(cuts))
        loudness = loudness * jnp.repeat(jnp.exp(heights), dims[position] // blocks).reshape((-1,) + (1,) * (len(dims) - 1 - position))
    return loudness


def gaussian(key, dims, width, reach, split=(), kind=jnp.bfloat16):
    entries = width * jax.random.normal(key, dims, jnp.float32)
    if split:
        entries = entries * steps_of(key, dims, split, -0.22, 0.18)
    return jnp.clip(entries, -reach, reach).astype(kind)


def setup_inputs(seed: int = 0) -> dict:
    streams_of = jax.random.split(jax.random.key(seed), 6)
    return {
        "ancestor_order": jax.vmap(lambda own: jax.random.permutation(own, NA))(jax.random.split(streams_of[0], NSUP)).reshape((NSUP, NA)).astype(jnp.int32),
        "factor_rows": gaussian(streams_of[1], (NSUP, NA * B, B), (NA * B) ** -0.5, 0.0390625, ((1, 32),)),
        "factor_inverse": draw_factor_inverse(jax.random.fold_in(streams_of[5], 71), 0),
        "ancestor_inverse": gaussian(streams_of[3], (NA * B, NA * B), 1.0, 6.0, ((0, 8), (1, 4))),
        "diagonal_inverse": gaussian(streams_of[4], (NSUP, B, B), 1.0, 6.0, ((2, 4),), jnp.float32),
    }


def reference(ancestor_order, factor_rows, factor_inverse, ancestor_inverse, diagonal_inverse):
    block_width = factor_rows.shape[2]
    chosen = ancestor_order[:, :NSEL]
    labels = jnp.arange(NA, dtype=jnp.int32)
    block_mask = jnp.any(chosen[:, :, None] == labels[None, None, :], axis=1).astype(jnp.float32)
    row_mask = jnp.repeat(block_mask, block_width, axis=1)
    offdiag_list = []
    diag_list = []
    for index in range(NSUP):
        normed = jnp.dot(factor_rows[index], factor_inverse[index], preferred_element_type=jnp.float32)
        normed = (normed * row_mask[index][:, None]).astype(jnp.bfloat16)
        product = jnp.dot(ancestor_inverse, normed, preferred_element_type=jnp.float32)
        offdiag_list.append((-(product * row_mask[index][:, None])).astype(jnp.bfloat16))
        correction = jnp.dot(normed.astype(jnp.float32).T, product, precision=lax.Precision.HIGHEST)
        diag_list.append(diagonal_inverse[index] + correction)
    return jnp.stack(offdiag_list), jnp.stack(diag_list)
```

```python
import functools

import jax
import jax.numpy as jnp
from jax import lax
from jax.experimental import pallas as pl
from jax.experimental.pallas import tpu as pltpu
from jax.sharding import PartitionSpec as P

NSEL = 40
MESH = pl.DeviceIdType.MESH


def kernel(
    dims, strips, own_ref, a_ref, out_ref, corr_ref,
    panel, abuf, acc, s1, r1, s2, r2, kept, below, cs, cr, total,
    own_sem, a_sem, ring_s, ring_r, s1s, r1s, s2s, r2s, bel_s, bel_r, bel_l, cs_s, cs_r, ag_s, ag_r,
):
    chips, n, depth = dims
    supers = own_ref.shape[0] // 2
    chunks = own_ref.shape[0]
    piece, wide = own_ref.shape[1], own_ref.shape[2]
    rows = acc.shape[1]
    width = wide // chips
    half = piece // 2
    tall = rows // 4
    per_slab = rows // piece
    slabs = n // per_slab
    r = lax.axis_index("row")
    c = lax.axis_index("col")
    x, k = r // 2, r % 2
    mate = x * 2 + 1 - k
    source_row = c // slabs
    source_x, source_k = source_row // 2, source_row % 2
    length = n // depth

    def col_at(pos):
        y, i = pos // length, pos % length
        return (i + (y % 2) * (length - 1 - 2 * i)) * depth + y

    y, z = c % depth, c // depth
    pos = y * length + z + (y % 2) * (length - 1 - 2 * z)
    right, left = col_at((pos + 1) % n), col_at((pos + n - 1) % n)

    def a_copy(i):
        src = place(i)[4]
        if strips:
            view = a_ref.at[src]
        else:
            view = a_ref.at[:, pl.ds(pl.multiple_of(src * piece, piece), piece)]
        return pltpu.make_async_copy(view, abuf.at[i % 2], a_sem.at[i % 2])

    def place(i):
        g, j = i // n, i % n
        t = (j + 1) // 2
        last = j // (n - 1)
        d = last * (g % 2) + (1 - last) * (1 - j % 2)
        return g, j, t, d, col_at((pos + (2 * d - 1) * t + n) % n)

    def ring(g, t, d, h, src):
        view = panel.at[g, src, pl.ds(h * half, half)]
        return pltpu.make_async_remote_copy(
            src_ref=view, dst_ref=view,
            send_sem=ring_s.at[d, g, t - 1, h], recv_sem=ring_r.at[d, g, t - 1, h],
            device_id=(r, right * (1 - d) + left * d), device_id_type=MESH,
        )

    def send_own(g):
        for h in range(2):
            for d in range(2):
                ring(g, 1, d, h, c).start()

    def below_copy(g, src, i, to_row, sem):
        return pltpu.make_async_remote_copy(
            src_ref=src, dst_ref=below.at[g, i], send_sem=sem, recv_sem=bel_r.at[g, i],
            device_id=(to_row, c), device_id_type=MESH,
        )

    def first_copy(s, b):
        return pltpu.make_async_remote_copy(
            src_ref=s1.at[s, b], dst_ref=r1.at[s, b], send_sem=s1s.at[s, b], recv_sem=r1s.at[s, b],
            device_id=(mate, c), device_id_type=MESH,
        )

    def second_copy(s, b, slot):
        return pltpu.make_async_remote_copy(
            src_ref=s2.at[s, b], dst_ref=r2.at[s, slot], send_sem=s2s.at[s, b], recv_sem=r2s.at[s, slot],
            device_id=(b * 2 + k, c), device_id_type=MESH,
        )

    def stage1(g):
        s = g // 2

        @pl.when(k != g % 2)
        def _():
            for b in range(chips):
                @pl.loop(0, 4)
                def _(m):
                    at = pl.ds(pl.multiple_of(m * tall, tall), tall)
                    s1[s, b, at, :] = acc[g % 2, at, pl.ds(b * width, width)].astype(jnp.bfloat16)
                first_copy(s, b).start()

    def stage2(g):
        s = g // 2

        @pl.when(k == g % 2)
        def _():
            for b in range(chips):
                first_copy(s, b).wait_recv()

                @pl.when(x == b)
                def _():
                    @pl.loop(0, 4)
                    def _(m):
                        at = pl.ds(pl.multiple_of(m * tall, tall), tall)
                        kept[s, at, :] = acc[g % 2, at, pl.ds(b * width, width)] + r1[s, b, at, :].astype(jnp.float32)

                @pl.when(x != b)
                def _():
                    @pl.loop(0, 4)
                    def _(m):
                        at = pl.ds(pl.multiple_of(m * tall, tall), tall)
                        both = acc[g % 2, at, pl.ds(b * width, width)] + r1[s, b, at, :].astype(jnp.float32)
                        s2[s, b, at, :] = both.astype(jnp.bfloat16)
                    second_copy(s, b, x).start()

    def stage3(g):
        s = g // 2

        @pl.when(k == g % 2)
        def _():
            for b in range(chips):
                @pl.when(x != b)
                def _():
                    second_copy(s, b, b).wait_recv()

                    @pl.loop(0, 4)
                    def _(m):
                        at = pl.ds(pl.multiple_of(m * tall, tall), tall)
                        kept[s, at, :] += r2[s, b, at, :].astype(jnp.float32)

            @pl.loop(0, 4)
            def _(m):
                at = pl.ds(pl.multiple_of(m * tall, tall), tall)
                out_ref[s, at, :] = kept[s, at, :].astype(jnp.bfloat16)

    def pass_below(g):
        @pl.when((k == source_k) & (x != source_x))
        def _():
            for i in range(per_slab):
                below_copy(g, below.at[g, i], i, mate, bel_s.at[g, i, chips]).wait_recv()
                below_copy(g, below.at[g, i], i, mate, bel_s.at[g, i, chips]).start()

    def local_own(g):
        return pltpu.make_async_copy(own_ref.at[g], panel.at[g, c], own_sem.at[g])

    for g in range(chunks):
        local_own(g).start()
    a_copy(0).start()
    barrier = pltpu.get_barrier_semaphore()
    for delta in range(1, n):
        pl.semaphore_signal(barrier, inc=1, device_id=(r, (c + delta) % n), device_id_type=MESH)
    pl.semaphore_signal(barrier, inc=1, device_id=(mate, c), device_id_type=MESH)
    for delta in range(1, chips):
        pl.semaphore_signal(barrier, inc=1, device_id=(((x + delta) % chips) * 2 + k, c), device_id_type=MESH)
    pl.semaphore_wait(barrier, n - 1 + 1 + chips - 1)
    for g in range(chunks):
        local_own(g).wait()
    send_own(0)

    @pl.loop(0, chunks * n)
    def _(i):
        g, j, t, d, src = place(i)

        @pl.when(j >= 1)
        def _():
            for h in range(2):
                ring(g, t, d, h, src).wait_recv()

                @pl.when((t + 1 < n // 2) | ((t + 1 == n // 2) & (d == g % 2)))
                def _():
                    ring(g, t + 1, d, h, src).start()

        @pl.when((j == n - 2) & (g < chunks - 1))
        def _():
            send_own(g + 1)

        @pl.when((r == source_row) & (src // per_slab == c % slabs))
        def _():
            at = src % per_slab
            for delta in range(1, chips):
                to = ((x + delta) % chips) * 2 + k
                below_copy(g, panel.at[g, src], at, to, bel_s.at[g, at, delta]).start()
            below_copy(g, panel.at[g, src], at, mate, bel_s.at[g, at, chips]).start()
            pltpu.make_async_copy(panel.at[g, src], below.at[g, at], bel_l.at[g, at]).start()

        a_copy(i).wait()

        @pl.when(i + 1 < chunks * n)
        def _():
            a_copy(i + 1).start()

        slot = i % 2

        @pl.loop(0, 4)
        def _(m):
            at = pl.ds(pl.multiple_of(m * tall, tall), tall)
            term = jnp.dot(abuf[slot, at, :], panel[g, src], preferred_element_type=jnp.float32)

            @pl.when(j == 0)
            def _():
                acc[g % 2, at, :] = term

            @pl.when(j > 0)
            def _():
                acc[g % 2, at, :] += term

        @pl.when(j == n - 1)
        def _():
            stage1(g)

        @pl.when((j == 1) & (g > 0))
        def _():
            stage2(g - 1)

        @pl.when((j == 3) & (g > 0))
        def _():
            pass_below(g - 1)

        @pl.when((j == n - 3) & (g > 0))
        def _():
            stage3(g - 1)

    stage2(chunks - 1)
    pass_below(chunks - 1)

    @pl.loop(0, chunks)
    def _(g):
        for i in range(per_slab):
            @pl.when(r == source_row)
            def _():
                pltpu.make_async_copy(panel.at[g, c], below.at[g, i], bel_l.at[g, i]).wait()

            @pl.when(k != source_k)
            def _():
                below_copy(g, below.at[g, i], i, mate, bel_s.at[g, i, chips]).wait_recv()

    stage3(chunks - 1)

    part = width // n

    @pl.loop(0, chunks)
    def _(g):
        term = jnp.zeros((width, wide), jnp.float32)
        for i in range(per_slab):
            term += lax.dot_general(
                out_ref[g // 2, pl.ds(i * piece, piece), :], below[g, i],
                (((0,), (0,)), ((), ())), preferred_element_type=jnp.float32,
            )
        for b in range(n):
            cs[b, g] = term[b * part:(b + 1) * part, :].astype(jnp.bfloat16)

    def scatter(delta):
        to = (c + delta) % n
        return pltpu.make_async_remote_copy(
            src_ref=cs.at[to], dst_ref=cr.at[delta], send_sem=cs_s.at[delta], recv_sem=cs_r.at[delta],
            device_id=(r, to), device_id_type=MESH,
        )

    def gather(delta, slot):
        return pltpu.make_async_remote_copy(
            src_ref=total, dst_ref=corr_ref.at[slot], send_sem=ag_s.at[delta], recv_sem=ag_r.at[delta],
            device_id=(r, (c + delta) % n), device_id_type=MESH,
        )

    for delta in range(1, n):
        scatter(delta).start()
    summed = cs[c].astype(jnp.float32)
    for delta in range(1, n):
        scatter(delta).wait_recv()
        summed += cr[delta].astype(jnp.float32)
    total[...] = summed.astype(jnp.bfloat16)
    for delta in range(1, n):
        gather(delta, c).start()
    corr_ref[c] = total[...]
    for delta in range(1, n):
        gather(delta, (c + n - delta) % n).wait_recv()

    for delta in range(1, n):
        scatter(delta).wait_send()
        gather(delta, c).wait_send()

    @pl.loop(0, chunks)
    def _(g):
        @pl.loop(1, n // 2 + 1)
        def _(t):
            for d in range(2):
                @pl.when((t < n // 2) | (d == g % 2))
                def _():
                    for h in range(2):
                        ring(g, t, d, h, c).wait_send()

        for i in range(per_slab):
            @pl.when(r == source_row)
            def _():
                for delta in range(1, chips):
                    below_copy(g, panel.at[g, c], i, mate, bel_s.at[g, i, delta]).wait_send()
                below_copy(g, panel.at[g, c], i, mate, bel_s.at[g, i, chips]).wait_send()

            @pl.when((k == source_k) & (x != source_x))
            def _():
                below_copy(g, below.at[g, i], i, mate, bel_s.at[g, i, chips]).wait_send()

    for s in range(supers):
        for b in range(chips):
            first_copy(s, b).wait_send()

            @pl.when(x != b)
            def _():
                second_copy(s, b, x).wait_send()


def body(ancestor_order, factor_rows, factor_inverse, ancestor_inverse, diagonal_inverse):
    supers, piece, block = factor_rows.shape
    rows = ancestor_inverse.shape[0]
    row_count, n = lax.axis_size("row"), lax.axis_size("col")
    r, c = lax.axis_index("row"), lax.axis_index("col")
    chips = row_count // 2
    depth = chips
    width = block // row_count
    wide = chips * width
    chunks = supers * 2
    chosen = ancestor_order[:, :NSEL]

    own_labels = ((r * n + c) * piece + jnp.arange(piece, dtype=jnp.int32)) // block
    own_keep = jnp.any(chosen[:, :, None] == own_labels[None, None, :], axis=1).astype(jnp.float32)
    inverse = factor_inverse.reshape(supers, block, chips, 2, width).transpose(0, 3, 1, 2, 4)
    inverse = inverse.reshape(supers, 2, block, wide)
    normed = jnp.einsum("srk,spkj->sprj", factor_rows, inverse, preferred_element_type=jnp.float32)
    normed = (normed * own_keep[:, None, :, None]).astype(jnp.bfloat16).reshape(chunks, piece, wide)

    strips = piece % 128 != 0
    left = ancestor_inverse
    if strips:
        left = left.reshape(rows, n, piece).transpose(1, 0, 2)
    per_slab = rows // piece
    part = width // n
    half_type, full_type, dma = jnp.bfloat16, jnp.float32, pltpu.SemaphoreType.DMA
    product, correction = pl.pallas_call(
        functools.partial(kernel, (chips, n, depth), strips),
        out_shape=(
            jax.ShapeDtypeStruct((supers, rows, width), half_type),
            jax.ShapeDtypeStruct((n, chunks, part, wide), half_type),
        ),
        in_specs=[pl.BlockSpec(memory_space=pl.ANY)] * 2,
        out_specs=(pl.BlockSpec(memory_space=pltpu.VMEM),) * 2,
        scratch_shapes=[
            pltpu.VMEM((chunks, n, piece, wide), half_type),
            pltpu.VMEM((2, rows, piece), half_type),
            pltpu.VMEM((2, rows, wide), full_type),
            pltpu.VMEM((supers, chips, rows, width), half_type),
            pltpu.VMEM((supers, chips, rows, width), half_type),
            pltpu.VMEM((supers, chips, rows, width), half_type),
            pltpu.VMEM((supers, chips, rows, width), half_type),
            pltpu.VMEM((supers, rows, width), full_type),
            pltpu.VMEM((chunks, per_slab, piece, wide), half_type),
            pltpu.VMEM((n, chunks, part, wide), half_type),
            pltpu.VMEM((n, chunks, part, wide), half_type),
            pltpu.VMEM((chunks, part, wide), half_type),
            dma((chunks,)),
            dma((2,)),
            dma((2, chunks, n // 2, 2)),
            dma((2, chunks, n // 2, 2)),
            dma((supers, chips)),
            dma((supers, chips)),
            dma((supers, chips)),
            dma((supers, chips)),
            dma((chunks, per_slab, chips + 1)),
            dma((chunks, per_slab)),
            dma((chunks, per_slab)),
            dma((n,)),
            dma((n,)),
            dma((n,)),
            dma((n,)),
        ],
        compiler_params=pltpu.CompilerParams(
            collective_id=0, has_side_effects=True, vmem_limit_bytes=64 * 1024 * 1024 - 65536
        ),
        cost_estimate=pl.CostEstimate(
            flops=2 * rows * n * piece * supers * block, bytes_accessed=8 * rows * n * piece, transcendentals=0
        ),
    )(normed, left)

    labels = (c * rows + jnp.arange(rows, dtype=jnp.int32)) // block
    keep = jnp.any(chosen[:, :, None] == labels[None, None, :], axis=1).astype(jnp.float32)
    offdiag = (-(product.astype(jnp.float32) * keep[:, :, None])).astype(jnp.bfloat16)
    correction = correction.astype(jnp.float32).reshape(n, supers, 2, part, chips, width)
    correction = correction.transpose(1, 4, 2, 5, 0, 3).reshape(supers, block, width)
    return offdiag, diagonal_inverse + correction


def solution(mesh):
    placed = (P(), P(None, ("row", "col"), None), P(), P("col", "row"), P(None, None, "row"))
    return jax.shard_map(
        body,
        mesh=mesh,
        in_specs=placed,
        out_specs=(P(None, "col", "row"), P(None, None, "row")),
        check_vma=False,
    )
```

```python
import functools

import jax
import jax.numpy as jnp
from jax import lax
from jax.experimental import pallas as pl
from jax.experimental.pallas import tpu as pltpu
from jax.sharding import PartitionSpec as P

NSEL = 40
MESH = pl.DeviceIdType.MESH


def kernel(
    dims, strips, order_ref, factor_ref, inverse_ref, a_ref, out_ref, corr_ref,
    panel, abuf, acc, s1, r1, s2, r2, kept, below, cs, cr, total,
    a_sem, ring_s, ring_r, s1s, r1s, s2s, r2s, bel_s, bel_r, bel_l, cs_s, cs_r, ag_s, ag_r,
):
    chips, n, depth = dims
    supers, piece, block = factor_ref.shape
    chunks = supers * 2
    rows, wide = acc.shape[1], acc.shape[2]
    width = wide // chips
    half = piece // 2
    tall = rows // 4
    per_slab = rows // piece
    slabs = n // per_slab
    r = lax.axis_index("row")
    c = lax.axis_index("col")
    x, k = r // 2, r % 2
    mate = x * 2 + 1 - k
    source_row = c // slabs
    source_x, source_k = source_row // 2, source_row % 2
    length = n // depth

    def col_at(pos):
        y, i = pos // length, pos % length
        return (i + (y % 2) * (length - 1 - 2 * i)) * depth + y

    y, z = c % depth, c // depth
    pos = y * length + z + (y % 2) * (length - 1 - 2 * z)
    right, left = col_at((pos + 1) % n), col_at((pos + n - 1) % n)

    def a_copy(i):
        src = place(i)[4]
        if strips:
            view = a_ref.at[src]
        else:
            view = a_ref.at[:, pl.ds(pl.multiple_of(src * piece, piece), piece)]
        return pltpu.make_async_copy(view, abuf.at[i % 2], a_sem.at[i % 2])

    def place(i):
        g, j = i // n, i % n
        t = (j + 1) // 2
        last = j // (n - 1)
        d = last * (g % 2) + (1 - last) * (1 - j % 2)
        return g, j, t, d, col_at((pos + (2 * d - 1) * t + n) % n)

    def ring(g, t, d, h, src):
        view = panel.at[g, src, pl.ds(h * half, half)]
        return pltpu.make_async_remote_copy(
            src_ref=view, dst_ref=view,
            send_sem=ring_s.at[d, g, t - 1, h], recv_sem=ring_r.at[d, g, t - 1, h],
            device_id=(r, right * (1 - d) + left * d), device_id_type=MESH,
        )

    def coupled(s, first, count):
        low = order_ref[pl.ds(s, 1), 0:NSEL] * block
        label = first + lax.broadcasted_iota(jnp.int32, (count, NSEL), 0)
        return jnp.sum(jnp.where((label >= low) & (label < low + block), 1.0, 0.0), axis=1, keepdims=True)

    def norm(g):
        s, p = g // 2, g % 2
        keep = coupled(s, (r * n + c) * piece, piece)
        for b in range(chips):
            at = pl.ds((2 * b + p) * width, width)
            term = jnp.dot(factor_ref[s], inverse_ref[s, :, at], preferred_element_type=jnp.float32)
            panel[g, c, :, pl.ds(b * width, width)] = (term * keep).astype(jnp.bfloat16)

    def below_copy(g, src, i, to_row, sem):
        return pltpu.make_async_remote_copy(
            src_ref=src, dst_ref=below.at[g, i], send_sem=sem, recv_sem=bel_r.at[g, i],
            device_id=(to_row, c), device_id_type=MESH,
        )

    def tile(m):
        return pl.ds(pl.multiple_of(m * tall, tall), tall)

    def first_copy(s, b, m):
        return pltpu.make_async_remote_copy(
            src_ref=s1.at[s, b, tile(m)], dst_ref=r1.at[s, b, tile(m)],
            send_sem=s1s.at[s, b, m], recv_sem=r1s.at[s, b, m],
            device_id=(mate, c), device_id_type=MESH,
        )

    def second_copy(s, b, m, slot):
        return pltpu.make_async_remote_copy(
            src_ref=s2.at[s, b, tile(m)], dst_ref=r2.at[s, slot, tile(m)],
            send_sem=s2s.at[s, b, m], recv_sem=r2s.at[s, slot, m],
            device_id=(b * 2 + k, c), device_id_type=MESH,
        )

    def stage1(g, m):
        s = g // 2
        for b in range(chips):
            s1[s, b, tile(m), :] = acc[g % 2, tile(m), pl.ds(b * width, width)].astype(jnp.bfloat16)
            first_copy(s, b, m).start()

    def stage2(g):
        s = g // 2

        @pl.when(k == g % 2)
        def _():
            @pl.loop(0, 4)
            def _(m):
                for b in range(chips):
                    first_copy(s, b, m).wait_recv()
                    both = acc[g % 2, tile(m), pl.ds(b * width, width)] + r1[s, b, tile(m), :].astype(jnp.float32)

                    @pl.when(x == b)
                    def _():
                        kept[s, tile(m), :] = both

                    @pl.when(x != b)
                    def _():
                        s2[s, b, tile(m), :] = both.astype(jnp.bfloat16)
                        second_copy(s, b, m, x).start()

    def stage3(g):
        s = g // 2

        @pl.when(k == g % 2)
        def _():
            @pl.loop(0, 4)
            def _(m):
                for b in range(chips):
                    @pl.when(x != b)
                    def _():
                        second_copy(s, b, m, b).wait_recv()
                        kept[s, tile(m), :] += r2[s, b, tile(m), :].astype(jnp.float32)
                keep = coupled(s, c * rows + m * tall, tall)
                out_ref[s, tile(m), :] = (-(kept[s, tile(m), :] * keep)).astype(jnp.bfloat16)

    def pass_below(g):
        @pl.when((k == source_k) & (x != source_x))
        def _():
            for i in range(per_slab):
                below_copy(g, below.at[g, i], i, mate, bel_s.at[g, i, chips]).wait_recv()
                below_copy(g, below.at[g, i], i, mate, bel_s.at[g, i, chips]).start()

    def scatter(s, delta):
        to = (c + delta) % n
        return pltpu.make_async_remote_copy(
            src_ref=cs.at[s, to], dst_ref=cr.at[s, delta],
            send_sem=cs_s.at[s, delta], recv_sem=cs_r.at[s, delta],
            device_id=(r, to), device_id_type=MESH,
        )

    def gather(s, delta, slot):
        return pltpu.make_async_remote_copy(
            src_ref=total.at[s], dst_ref=corr_ref.at[s, slot],
            send_sem=ag_s.at[s, delta], recv_sem=ag_r.at[s, delta],
            device_id=(r, (c + delta) % n), device_id_type=MESH,
        )

    def wait_below(s):
        for q in range(2):
            for i in range(per_slab):
                g = 2 * s + q

                @pl.when(r == source_row)
                def _():
                    pltpu.make_async_copy(panel.at[g, c], below.at[g, i], bel_l.at[g, i]).wait()

                @pl.when(k != source_k)
                def _():
                    below_copy(g, below.at[g, i], i, mate, bel_s.at[g, i, chips]).wait_recv()

    def correct(s):
        for q in range(2):
            term = jnp.zeros((width, wide), jnp.float32)
            for i in range(per_slab):
                term -= lax.dot_general(
                    out_ref[s, pl.ds(i * piece, piece), :], below[2 * s + q, i],
                    (((0,), (0,)), ((), ())), preferred_element_type=jnp.float32,
                )
            for b in range(n):
                cs[s, b, q] = term[b * part:(b + 1) * part, :].astype(jnp.bfloat16)
        for delta in range(1, n):
            scatter(s, delta).start()

    def collect(s):
        summed = cs[s, c].astype(jnp.float32)
        for delta in range(1, n):
            scatter(s, delta).wait_recv()
            summed += cr[s, delta].astype(jnp.float32)
        total[s] = summed.astype(jnp.bfloat16)
        for delta in range(1, n):
            gather(s, delta, c).start()
        corr_ref[s, c] = summed.astype(jnp.bfloat16)

    part = width // n
    barrier = pltpu.get_barrier_semaphore()
    for delta in range(1, n):
        pl.semaphore_signal(barrier, inc=1, device_id=(r, (c + delta) % n), device_id_type=MESH)
    pl.semaphore_signal(barrier, inc=1, device_id=(mate, c), device_id_type=MESH)
    for delta in range(1, chips):
        pl.semaphore_signal(barrier, inc=1, device_id=(((x + delta) % chips) * 2 + k, c), device_id_type=MESH)
    a_copy(0).start()
    norm(0)
    pl.semaphore_wait(barrier, n - 1 + 1 + chips - 1)
    for h in range(2):
        for d in range(2):
            ring(0, 1, d, h, c).start()
    for g in range(1, chunks):
        norm(g)

    @pl.loop(0, chunks * n)
    def _(i):
        g, j, t, d, src = place(i)

        ahead, h = j // 2 + 1, j % 2
        for way in range(2):
            @pl.when((ahead < n // 2) | (way == g % 2))
            def _():
                come = col_at((pos + (2 * way - 1) * ahead + n) % n)
                ring(g, ahead, way, h, come).wait_recv()

                @pl.when((ahead + 1 < n // 2) | ((ahead + 1 == n // 2) & (way == g % 2)))
                def _():
                    ring(g, ahead + 1, way, h, come).start()

            @pl.when((g < chunks - 1) & (j == n - 5 + 2 * ((g + way + 1) % 2)))
            def _():
                for first in range(2):
                    ring(g + 1, 1, way, first, c).start()

        @pl.when((r == source_row) & (src // per_slab == c % slabs))
        def _():
            at = src % per_slab
            for delta in range(1, chips):
                to = ((x + delta) % chips) * 2 + k
                below_copy(g, panel.at[g, src], at, to, bel_s.at[g, at, delta]).start()
            below_copy(g, panel.at[g, src], at, mate, bel_s.at[g, at, chips]).start()
            pltpu.make_async_copy(panel.at[g, src], below.at[g, at], bel_l.at[g, at]).start()

        a_copy(i).wait()

        @pl.when(i + 1 < chunks * n)
        def _():
            a_copy(i + 1).start()

        slot = i % 2

        @pl.loop(0, 4)
        def _(m):
            at = pl.ds(pl.multiple_of(m * tall, tall), tall)
            term = jnp.dot(abuf[slot, at, :], panel[g, src], preferred_element_type=jnp.float32)

            @pl.when(j == 0)
            def _():
                acc[g % 2, at, :] = term

            @pl.when(j > 0)
            def _():
                acc[g % 2, at, :] += term

            @pl.when((j == n - 1) & (k != g % 2))
            def _():
                stage1(g, m)

        @pl.when((j == 1) & (g > 0))
        def _():
            stage2(g - 1)

        @pl.when((j == 3) & (g > 0))
        def _():
            pass_below(g - 1)

        @pl.when((j == n - 3) & (g > 0))
        def _():
            stage3(g - 1)

        @pl.when((j == 2) & (g >= 3) & (g % 2 == 1))
        def _():
            wait_below((g - 3) // 2)
            correct((g - 3) // 2)

        @pl.when((j == n - 2) & (g >= 3) & (g % 2 == 1))
        def _():
            collect((g - 3) // 2)

    stage2(chunks - 1)
    pass_below(chunks - 1)
    wait_below(supers - 1)
    stage3(chunks - 1)
    correct(supers - 1)
    collect(supers - 1)
    for s in range(supers):
        for delta in range(1, n):
            gather(s, delta, (c + n - delta) % n).wait_recv()
            scatter(s, delta).wait_send()
            gather(s, delta, c).wait_send()

    @pl.loop(0, chunks)
    def _(g):
        @pl.loop(1, n // 2 + 1)
        def _(t):
            for d in range(2):
                @pl.when((t < n // 2) | (d == g % 2))
                def _():
                    for h in range(2):
                        ring(g, t, d, h, c).wait_send()

        for i in range(per_slab):
            @pl.when(r == source_row)
            def _():
                for delta in range(1, chips):
                    below_copy(g, panel.at[g, c], i, mate, bel_s.at[g, i, delta]).wait_send()
                below_copy(g, panel.at[g, c], i, mate, bel_s.at[g, i, chips]).wait_send()

            @pl.when((k == source_k) & (x != source_x))
            def _():
                below_copy(g, below.at[g, i], i, mate, bel_s.at[g, i, chips]).wait_send()

    for s in range(supers):
        for b in range(chips):
            @pl.loop(0, 4)
            def _(m):
                first_copy(s, b, m).wait_send()

                @pl.when(x != b)
                def _():
                    second_copy(s, b, m, x).wait_send()


def body(ancestor_order, factor_rows, factor_inverse, ancestor_inverse, diagonal_inverse):
    supers, piece, block = factor_rows.shape
    rows = ancestor_inverse.shape[0]
    row_count, n = lax.axis_size("row"), lax.axis_size("col")
    chips = row_count // 2
    depth = chips
    width = block // row_count
    wide = chips * width
    chunks = supers * 2

    strips = piece % 128 != 0
    left = ancestor_inverse
    if strips:
        left = left.reshape(rows, n, piece).transpose(1, 0, 2)
    per_slab = rows // piece
    part = width // n
    half_type, full_type, dma = jnp.bfloat16, jnp.float32, pltpu.SemaphoreType.DMA
    offdiag, correction = pl.pallas_call(
        functools.partial(kernel, (chips, n, depth), strips),
        out_shape=(
            jax.ShapeDtypeStruct((supers, rows, width), half_type),
            jax.ShapeDtypeStruct((supers, n, 2, part, wide), half_type),
        ),
        in_specs=[pl.BlockSpec(memory_space=pltpu.VMEM)] * 3 + [pl.BlockSpec(memory_space=pl.ANY)],
        out_specs=(pl.BlockSpec(memory_space=pltpu.VMEM),) * 2,
        scratch_shapes=[
            pltpu.VMEM((chunks, n, piece, wide), half_type),
            pltpu.VMEM((2, rows, piece), half_type),
            pltpu.VMEM((2, rows, wide), full_type),
            pltpu.VMEM((supers, chips, rows, width), half_type),
            pltpu.VMEM((supers, chips, rows, width), half_type),
            pltpu.VMEM((supers, chips, rows, width), half_type),
            pltpu.VMEM((supers, chips, rows, width), half_type),
            pltpu.VMEM((supers, rows, width), full_type),
            pltpu.VMEM((chunks, per_slab, piece, wide), half_type),
            pltpu.VMEM((supers, n, 2, part, wide), half_type),
            pltpu.VMEM((supers, n, 2, part, wide), half_type),
            pltpu.VMEM((supers, 2, part, wide), half_type),
            dma((2,)),
            dma((2, chunks, n // 2, 2)),
            dma((2, chunks, n // 2, 2)),
            dma((supers, chips, 4)),
            dma((supers, chips, 4)),
            dma((supers, chips, 4)),
            dma((supers, chips, 4)),
            dma((chunks, per_slab, chips + 1)),
            dma((chunks, per_slab)),
            dma((chunks, per_slab)),
            dma((supers, n)),
            dma((supers, n)),
            dma((supers, n)),
            dma((supers, n)),
        ],
        compiler_params=pltpu.CompilerParams(
            collective_id=0, has_side_effects=True, vmem_limit_bytes=64 * 1024 * 1024 - 65536
        ),
        cost_estimate=pl.CostEstimate(
            flops=2 * rows * n * piece * supers * block, bytes_accessed=8 * rows * n * piece, transcendentals=0
        ),
    )(ancestor_order, factor_rows, factor_inverse, left)

    correction = correction.astype(jnp.float32).reshape(supers, n, 2, part, chips, width)
    correction = correction.transpose(0, 4, 2, 5, 1, 3).reshape(supers, block, width)
    return offdiag, diagonal_inverse + correction


def solution(mesh):
    placed = (P(), P(None, ("row", "col"), None), P(), P("col", "row"), P(None, None, "row"))
    return jax.shard_map(
        body,
        mesh=mesh,
        in_specs=placed,
        out_specs=(P(None, "col", "row"), P(None, None, "row")),
        check_vma=False,
    )
```
